32 devices in a mesh: ctx: 8 (over z, y), dp: 4 (over x, core).
Axes of the slice: x: 2, y: 2, z: 4, core: 2. Of those that a mesh axis runs over, the one named last changes fastest.
Arguments:
- tokens: bfloat16 [8, 512, 4096], P('dp', 'ctx'), may hold values from -6 to 6
- queries: bfloat16 [8, 512, 2048], P('dp', 'ctx'), may hold values from -160 to 160
- d_attended: bfloat16 [8, 512, 2048], P('dp', 'ctx'), may hold values from -6 to 6
- span_order: int32 [16], replicated, may hold values from 0 to 15, each once
- norm_gain: float32 [4096], replicated, may hold values from 0.1 to 1.9
- key_weight: bfloat16 [4096, 512], replicated, may hold values from -0.09375 to 0.09375
- value_weight: bfloat16 [4096, 512], replicated, may hold values from -0.09375 to 0.09375
Outputs:
- attended: bfloat16 [8, 512, 2048], P('dp', 'ctx')
- grad_queries: bfloat16 [8, 512, 2048], P('dp', 'ctx')
- grad_tokens: bfloat16 [8, 512, 4096], P('dp', 'ctx')
- grad_key_weight: float32 [4096, 512], P(('ctx', 'dp'))
- grad_value_weight: float32 [4096, 512], P(('ctx', 'dp'))
- grad_gain: float32 [4096], P(('ctx', 'dp'))
The draws below stay inside these ranges and needn't reach their ends.
All inputs are finite; a program needn't handle non-finite values.
Results may differ from the reference program's by a relative error of at most 0.025.
The reference program's roundings to bfloat16 on the way (of `normed`, `rotated_keys`, `value_rows`, `probability_b`, `dscores`, `key_pre_grad` and `value_pre_grad`) count: a program that leaves them out, or rounds other values in their place, can miss the bound.
Values may be sent and summed in bfloat16 or wider, within the bound.
A program may use at most 192 MiB of HBM per device.

```python
import jax
import jax.numpy as jnp
from jax import lax

D = 4096
HEADS = 16
KV_HEADS = 4
HEAD_DIM = 128
SEQ_DEV = 64
SEQ = 512
SEQS = 8
N_CTX = 8


def draw_queries(key, part):
    full_shape = (SEQS, SEQ, HEADS * HEAD_DIM)
    sample = jnp.clip(jax.random.normal(key, full_shape, jnp.float32), -4.0, 4.0)
    return sample.astype(jnp.bfloat16)


def shard_levels(own_key, extent, shards, smallest, largest):
    factor_of = 1.0
    for axis_at, parts in shards:
        heights = jax.random.uniform(jax.random.fold_in(jax.random.fold_in(own_key, 6), axis_at), (parts,), jnp.float32, smallest / len(shards), largest / len(shards))
        factor_of = factor_of * jnp.repeat(jnp.exp(heights), extent[axis_at] // parts).reshape((-1,) + (1,) * (len(extent) - 1 - axis_at))
    return factor_of


def gaussian(key, shape, scale, limit, shards=(), kind=jnp.bfloat16):
    factor_of = shard_levels(key, shape, shards, -0.22, 0.18) if shards else 1.0
    entries = jax.random.normal(key, shape, jnp.float32) * scale * factor_of
    return jnp.minimum(jnp.maximum(entries, -limit), limit).astype(kind)


def setup_inputs(seed: int = 0) -> dict:
    arg_keys = jax.random.split(jax.random.key(seed), 8)
    return {
        "tokens": gaussian(arg_keys[0], (SEQS, SEQ, D), 1.0, 6.0, ((0, 4), (1, 8))),
        "queries": draw_queries(jax.random.fold_in(arg_keys[7], 71), 0),
        "d_attended": gaussian(arg_keys[2], (SEQS, SEQ, HEADS * HEAD_DIM), 1.0, 6.0, ((0, 4), (1, 8))),
        "span_order": jax.random.permutation(arg_keys[3], 2 * N_CTX).astype(jnp.int32),
        "norm_gain": jnp.clip(1.0 + 0.18 * jax.random.normal(arg_keys[4], (D,), jnp.float32), 0.1, 1.9),
        "key_weight": gaussian(arg_keys[5], (D, KV_HEADS * HEAD_DIM), D ** -0.5, 0.09375),
        "value_weight": gaussian(arg_keys[6], (D, KV_HEADS * HEAD_DIM), D ** -0.5, 0.09375),
    }


ROPE_BASE = 500000.0
EPSILON = 1e-05

def positions(span_order, span_len):
    offsets = jnp.arange(span_len, dtype=jnp.int32)
    return (span_order[:, None] * span_len + offsets[None, :]).reshape(-1).astype(jnp.int32)

def rotation(token_pos, head_size):
    half_dim = head_size // 2
    frequency = ROPE_BASE ** (-2.0 * jnp.arange(half_dim, dtype=jnp.float32) / head_size)
    angles = token_pos.astype(jnp.float32)[:, None] * frequency[None, :]
    angles = jnp.concatenate([angles, angles], axis=1)
    return (jnp.cos(angles), jnp.sin(angles))

def rotate_half(values):
    half_dim = values.shape[-1] // 2
    return jnp.concatenate([-values[..., half_dim:], values[..., :half_dim]], axis=-1)

def rotate_back(values):
    half_dim = values.shape[-1] // 2
    return jnp.concatenate([values[..., half_dim:], -values[..., :half_dim]], axis=-1)

def normalize(tokens, norm_gain):
    widened = tokens.astype(jnp.float32)
    rms_scale = lax.rsqrt(lax.optimization_barrier(jnp.mean(widened * widened, axis=-1, keepdims=True)) + EPSILON)
    return ((widened * rms_scale * norm_gain).astype(jnp.bfloat16), rms_scale)

def project_keys(normed, key_weight, value_weight, cosine, sine_table, kv_heads, head_size):
    row_count = normed.shape[0]
    key_pre = jnp.dot(normed, key_weight, preferred_element_type=jnp.float32).reshape(row_count, kv_heads, head_size)
    rotated = key_pre * cosine[:, None, :] + rotate_half(key_pre) * sine_table[:, None, :]
    value_rows = jnp.dot(normed, value_weight, preferred_element_type=jnp.float32)
    return (rotated.reshape(row_count, kv_heads * head_size).astype(jnp.bfloat16), value_rows.astype(jnp.bfloat16))

def attend_group(query_group, grad_group, key_group, value_group, causal_mask, score_scale):
    query_wide = query_group.astype(jnp.float32)
    grad_wide = grad_group.astype(jnp.float32)
    key_wide = key_group.astype(jnp.float32)
    value_wide = value_group.astype(jnp.float32)
    scores = jnp.einsum('tgd,sd->gts', query_wide, key_wide) * score_scale
    scores = jnp.where(causal_mask[None], scores, -1e+30)
    row_max = lax.optimization_barrier(jnp.max(scores, axis=-1, keepdims=True))
    exponent = jnp.exp(scores - row_max)
    probability = exponent / lax.optimization_barrier(jnp.sum(exponent, axis=-1, keepdims=True))
    probability_b = probability.astype(jnp.bfloat16)
    prob_wide = probability_b.astype(jnp.float32)
    attended = jnp.einsum('gts,sd->tgd', prob_wide, value_wide).astype(jnp.bfloat16)
    dprob = jnp.einsum('tgd,sd->gts', grad_wide, value_wide)
    delta = lax.optimization_barrier(jnp.sum(grad_wide * attended.astype(jnp.float32), axis=-1))
    dscores = (probability * (dprob - jnp.transpose(delta)[:, :, None])).astype(jnp.bfloat16)
    dscore_wide = dscores.astype(jnp.float32)
    dquery = (jnp.einsum('gts,sd->tgd', dscore_wide, key_wide) * score_scale).astype(jnp.bfloat16)
    key_term = jnp.einsum('gts,tgd->sd', dscore_wide, query_wide) * score_scale
    value_term = jnp.einsum('gts,tgd->sd', prob_wide, grad_wide)
    return (attended, dquery, key_term, value_term)

def attend_device(queries, grads, all_keys, all_values, query_pos, key_pos, kv_heads, head_size):
    row_count = queries.shape[0]
    group_size = queries.shape[1] // (kv_heads * head_size)
    group_width = group_size * head_size
    causal_mask = key_pos[None, :] <= query_pos[:, None]
    score_scale = head_size ** (-0.5)
    outputs = []
    for head_group in range(kv_heads):
        query_group = queries[:, head_group * group_width:(head_group + 1) * group_width].reshape(row_count, group_size, head_size)
        grad_group = grads[:, head_group * group_width:(head_group + 1) * group_width].reshape(row_count, group_size, head_size)
        key_group = all_keys[:, head_group * head_size:(head_group + 1) * head_size]
        value_group = all_values[:, head_group * head_size:(head_group + 1) * head_size]
        outputs.append(attend_group(query_group, grad_group, key_group, value_group, causal_mask, score_scale))
    attended = jnp.concatenate([item[0].reshape(row_count, group_width) for item in outputs], axis=1)
    dquery = jnp.concatenate([item[1].reshape(row_count, group_width) for item in outputs], axis=1)
    key_terms = jnp.concatenate([item[2] for item in outputs], axis=1)
    value_terms = jnp.concatenate([item[3] for item in outputs], axis=1)
    return (attended, dquery, key_terms, value_terms)

def finish_backward(tokens, normed, rms_scale, key_grad, value_grad, cosine, sine_table, norm_gain, key_weight, value_weight, kv_heads, head_size):
    row_count = tokens.shape[0]
    shaped = key_grad.reshape(row_count, kv_heads, head_size)
    key_pre_grad = (shaped * cosine[:, None, :] + rotate_back(shaped * sine_table[:, None, :])).reshape(row_count, kv_heads * head_size).astype(jnp.bfloat16)
    value_pre_grad = value_grad.astype(jnp.bfloat16)
    weight_key = jnp.dot(normed.T, key_pre_grad, preferred_element_type=jnp.float32)
    weight_value = jnp.dot(normed.T, value_pre_grad, preferred_element_type=jnp.float32)
    normed_grad = jnp.dot(key_pre_grad, key_weight.T, preferred_element_type=jnp.float32) + jnp.dot(value_pre_grad, value_weight.T, preferred_element_type=jnp.float32)
    widened = tokens.astype(jnp.float32)
    gain_part = lax.optimization_barrier(jnp.sum(normed_grad * widened * rms_scale, axis=0))
    inner_mean = lax.optimization_barrier(jnp.mean(normed_grad * norm_gain * widened, axis=-1, keepdims=True))
    grad_rows = (rms_scale * norm_gain * normed_grad - widened * rms_scale ** 3 * inner_mean).astype(jnp.bfloat16)
    return (grad_rows, weight_key, weight_value, gain_part)

def reference(tokens, queries, d_attended, span_order, norm_gain, key_weight, value_weight):
    token_pos = positions(span_order, SEQ_DEV // 2)
    cosine, sine_table = rotation(token_pos, HEAD_DIM)
    kv_width = KV_HEADS * HEAD_DIM
    total_key = jnp.zeros((D, kv_width), jnp.float32)
    total_value = jnp.zeros((D, kv_width), jnp.float32)
    total_gain = jnp.zeros((D,), jnp.float32)
    attended_list, dquery_list, dtoken_list = ([], [], [])
    for sequence in range(SEQS):
        normed, rms_scale = normalize(tokens[sequence], norm_gain)
        rotated_keys, value_rows = project_keys(normed, key_weight, value_weight, cosine, sine_table, KV_HEADS, HEAD_DIM)
        seq_queries = queries[sequence]
        seq_grads = d_attended[sequence]

        def shard_step(totals, shard_index):
            first_row = shard_index * SEQ_DEV
            block_queries = lax.dynamic_slice_in_dim(seq_queries, first_row, SEQ_DEV, 0)
            block_grads = lax.dynamic_slice_in_dim(seq_grads, first_row, SEQ_DEV, 0)
            query_pos = lax.dynamic_slice_in_dim(token_pos, first_row, SEQ_DEV, 0)
            attended, dquery, key_terms, value_terms = attend_device(block_queries, block_grads, rotated_keys, value_rows, query_pos, token_pos, KV_HEADS, HEAD_DIM)
            key_round = lax.optimization_barrier(key_terms.astype(jnp.bfloat16)).astype(jnp.float32)
            value_round = lax.optimization_barrier(value_terms.astype(jnp.bfloat16)).astype(jnp.float32)
            return ((totals[0] + key_round, totals[1] + value_round), (attended, dquery))
        zeros_init = jnp.zeros((SEQ, kv_width), jnp.float32)
        sums, stacked = lax.scan(shard_step, (zeros_init, zeros_init), jnp.arange(N_CTX, dtype=jnp.int32))
        attended_list.append(stacked[0].reshape(SEQ, HEADS * HEAD_DIM))
        dquery_list.append(stacked[1].reshape(SEQ, HEADS * HEAD_DIM))
        grad_rows, weight_key, weight_value, gain_part = finish_backward(tokens[sequence], normed, rms_scale, sums[0], sums[1], cosine, sine_table, norm_gain, key_weight, value_weight, KV_HEADS, HEAD_DIM)
        dtoken_list.append(grad_rows)
        total_key = total_key + weight_key
        total_value = total_value + weight_value
        total_gain = total_gain + gain_part
    return (jnp.stack(attended_list), jnp.stack(dquery_list), jnp.stack(dtoken_list), total_key, total_value, total_gain)
```

```python
import functools

import jax
import jax.numpy as jnp
from jax import lax
from jax.experimental import pallas as pl
from jax.experimental.pallas import tpu as pltpu
from jax.sharding import PartitionSpec as P

KV_HEADS = 4
HEAD_DIM = 128
ROPE_BASE = 500000.0
EPSILON = 1e-05
MESH = pl.DeviceIdType.MESH
VMEM = pl.BlockSpec(memory_space=pltpu.VMEM)
F32 = jnp.float32
BF16 = jnp.bfloat16
LIMIT = 60 * 1024 * 1024


def positions(span_order, span_len):
    offsets = jnp.arange(span_len, dtype=jnp.int32)
    return (span_order[:, None] * span_len + offsets[None, :]).reshape(-1)


def rotation(token_pos, head_size):
    half_dim = head_size // 2
    frequency = ROPE_BASE ** (-2.0 * jnp.arange(half_dim, dtype=F32) / head_size)
    angles = token_pos.astype(F32)[:, None] * frequency[None, :]
    angles = jnp.concatenate([angles, angles], axis=1)
    return (jnp.cos(angles), jnp.sin(angles))


def ring_place(index, n):
    return jnp.where(index % 2 == 0, index // 2, n - 1 - index // 2)


def ring_index(place, n):
    place = (place + 2 * n) % n
    return jnp.where(place < n // 2, 2 * place, 2 * (n - 1 - place) + 1)


def remote(src, dst, send, recv, axis, target):
    return pltpu.make_async_remote_copy(
        src_ref=src,
        dst_ref=dst,
        send_sem=send,
        recv_sem=recv,
        device_id={axis: target},
        device_id_type=MESH,
    )


def greet(axis, n, me):
    barrier = pltpu.get_barrier_semaphore()
    for j in range(1, n):
        pl.semaphore_signal(
            barrier, inc=1, device_id={axis: (me + j) % n}, device_id_type=MESH
        )
    pl.semaphore_wait(barrier, n - 1)


def ring_gather(n, me, firsts, alls, send, recv, extra=None):
    place = ring_place(me, n)
    sign = (1, -1)
    targets = [ring_index(place + 1, n), ring_index(place - 1, n)]
    chunks = firsts[0].shape[0]

    def copy(d, c, s, first=False):
        owner = ring_index(place - sign[d] * s, n)
        src = firsts[d].at[c] if first else alls[d].at[owner, c]
        return remote(
            src, alls[d].at[owner, c], send.at[d, c, s], recv.at[d, c, s], "ctx", targets[d]
        )

    def arrive(d, c, s):
        owner = ring_index(place - sign[d] * (s + 1), n)
        slot = alls[d].at[owner, c]
        remote(slot, slot, send.at[d, c, s], recv.at[d, c, s], "ctx", targets[d]).wait_recv()

    for c in range(chunks):
        for d in range(2):
            copy(d, c, 0, first=True).start()

    def step(s, carry):
        for c in range(chunks):
            for d in range(2):
                arrive(d, c, s)
                copy(d, c, s + 1).start()
        if extra is not None:
            extra(s + 1)
        return carry

    if extra is not None:
        extra(0)
    lax.fori_loop(0, n - 2, step, 0)
    for c in range(chunks):
        for d in range(2):
            arrive(d, c, n - 2)

    def drain(s, carry):
        for c in range(chunks):
            for d in range(2):
                copy(d, c, s).wait_send()
        return carry

    lax.fori_loop(0, n - 1, drain, 0)


def gather_kernel(n, k_ref, v_ref, a_ref, gk, gv, ga, send, recv, asend, arecv):
    me = lax.axis_index("ctx")
    width = ga.shape[2]
    greet("ctx", n, me)
    gk[me] = k_ref[...]
    gv[me] = v_ref[...]
    ga[me] = a_ref[:, pl.ds(pl.multiple_of(me * width, 128), width)]

    def piece(j):
        target = (me + j) % n
        return remote(
            a_ref.at[:, pl.ds(pl.multiple_of(target * width, 128), width)],
            ga.at[me],
            asend.at[j - 1],
            arecv.at[j - 1],
            "ctx",
            target,
        )

    ring_gather(n, me, (k_ref, v_ref), (gk, gv), send, recv, lambda s: piece(s + 1).start())

    def finish(j, carry):
        piece(j).wait_send()
        slot = ga.at[(me + n - j) % n]
        remote(slot, slot, asend.at[j - 1], arecv.at[j - 1], "ctx", (me + j) % n).wait_recv()
        return carry

    lax.fori_loop(1, n, finish, 0)


def gather(n, keys, values, normed):
    seqs = keys.shape[0]
    kv = jax.ShapeDtypeStruct((n,) + keys.shape, BF16)
    return pl.pallas_call(
        functools.partial(gather_kernel, n),
        out_shape=(
            kv,
            kv,
            jax.ShapeDtypeStruct((n, normed.shape[0], normed.shape[1] // n), BF16),
        ),
        in_specs=[VMEM] * 3,
        out_specs=[VMEM] * 3,
        scratch_shapes=[
            pltpu.SemaphoreType.DMA((2, seqs, n - 1)),
            pltpu.SemaphoreType.DMA((2, seqs, n - 1)),
            pltpu.SemaphoreType.DMA((n - 1,)),
            pltpu.SemaphoreType.DMA((n - 1,)),
        ],
        compiler_params=pltpu.CompilerParams(
            collective_id=0, has_side_effects=True, vmem_limit_bytes=LIMIT
        ),
        name="gather_kv",
    )(keys, values, normed)


def attention_kernel(q_ref, g_ref, k_ref, v_ref, qpos_ref, kpos_ref, att, dq, dk, dv):
    n, _, rows, head = k_ref.shape
    group = q_ref.shape[2] // head
    scale = head ** (-0.5)
    query = jnp.concatenate([q_ref[0, :, i * head : (i + 1) * head] for i in range(group)], axis=0)
    grad = jnp.concatenate([g_ref[0, :, i * head : (i + 1) * head] for i in range(group)], axis=0)
    key = k_ref[...].reshape(n * rows, head)
    value = v_ref[...].reshape(n * rows, head)
    nt = (((1,), (1,)), ((), ()))
    nn = (((1,), (0,)), ((), ()))
    tn = (((0,), (0,)), ((), ()))
    dot = functools.partial(lax.dot_general, preferred_element_type=F32)
    keep = kpos_ref[...] <= jnp.concatenate([qpos_ref[...]] * group, axis=0)
    scores = jnp.where(keep, dot(query, key, nt) * scale, -1e30)
    exponent = jnp.exp(scores - jnp.max(scores, axis=1, keepdims=True))
    probability = exponent * (1.0 / jnp.sum(exponent, axis=1, keepdims=True))
    rounded = probability.astype(BF16)
    attended = dot(rounded, value, nn).astype(BF16)
    delta = jnp.sum(grad.astype(F32) * attended.astype(F32), axis=1, keepdims=True)
    dscores = (probability * (dot(grad, value, nt) - delta)).astype(BF16)
    dquery = (dot(dscores, key, nn) * scale).astype(BF16)
    for i in range(group):
        att[0, :, i * head : (i + 1) * head] = attended[i * rows : (i + 1) * rows]
        dq[0, :, i * head : (i + 1) * head] = dquery[i * rows : (i + 1) * rows]
    dk[...] = (dot(dscores, query, tn) * scale).astype(BF16).reshape(n, 1, rows, head)
    dv[...] = dot(rounded, grad, tn).astype(BF16).reshape(n, 1, rows, head)


def attention(queries, grads, all_keys, all_values, query_pos, key_pos):
    n, seqs, rows, width = all_keys.shape
    kv_heads = width // HEAD_DIM
    wide = pl.BlockSpec((1, rows, queries.shape[2] // kv_heads), lambda s, h: (s, 0, h))
    narrow = pl.BlockSpec((n, 1, rows, HEAD_DIM), lambda s, h: (0, s, 0, h))
    return pl.pallas_call(
        attention_kernel,
        grid=(seqs, kv_heads),
        out_shape=(
            jax.ShapeDtypeStruct(queries.shape, BF16),
            jax.ShapeDtypeStruct(queries.shape, BF16),
            jax.ShapeDtypeStruct(all_keys.shape, BF16),
            jax.ShapeDtypeStruct(all_keys.shape, BF16),
        ),
        in_specs=[
            wide,
            wide,
            narrow,
            narrow,
            pl.BlockSpec((rows, 1), lambda s, h: (0, 0)),
            pl.BlockSpec((1, n * rows), lambda s, h: (0, 0)),
        ],
        out_specs=[wide, wide, narrow, narrow],
        compiler_params=pltpu.CompilerParams(vmem_limit_bytes=LIMIT),
        name="attention",
    )(queries, grads, all_keys, all_values, query_pos[:, None], key_pos[None, :])


def reduce_kernel(n, dk, dv, cos_ref, sin_ref, gk, gv, ik, iv, own_k, own_v, rs, rr, send, recv):
    me = lax.axis_index("ctx")
    place = ring_place(me, n)
    seqs = dk.shape[1]
    sign = (1, -1)
    targets = [ring_index(place + 1, n), ring_index(place - 1, n)]
    terms = (dk, dv)
    inbox = (ik, iv)
    greet("ctx", n, me)

    def copy(d, c, s, first=False):
        src = terms[d].at[targets[1 - d], c] if first else inbox[d].at[s - 1, c]
        return remote(src, inbox[d].at[s, c], rs.at[d, c, s], rr.at[d, c, s], "ctx", targets[d])

    def total(d, c, s):
        slot = inbox[d].at[s, c]
        remote(slot, slot, rs.at[d, c, s], rr.at[d, c, s], "ctx", targets[d]).wait_recv()
        owner = ring_index(place - sign[d] * (s + 2), n)
        return inbox[d][s, c].astype(F32) + terms[d][owner, c].astype(F32)

    for c in range(seqs):
        for d in range(2):
            copy(d, c, 0, first=True).start()

    def step(s, carry):
        for c in range(seqs):
            for d in range(2):
                inbox[d][s, c] = total(d, c, s).astype(BF16)
                copy(d, c, s + 1).start()
        return carry

    lax.fori_loop(0, n - 2, step, 0)
    for c in range(seqs):
        key_grad = total(0, c, n - 2)
        for h in range(key_grad.shape[1] // HEAD_DIM):
            part = key_grad[:, h * HEAD_DIM : (h + 1) * HEAD_DIM]
            turned = pltpu.roll(part, HEAD_DIM // 2, 1)
            back = (part * cos_ref[...] + turned * sin_ref[...]).astype(BF16)
            own_k[c, :, h * HEAD_DIM : (h + 1) * HEAD_DIM] = back
        own_v[c] = total(1, c, n - 2).astype(BF16)
    gk[me] = own_k[...]
    gv[me] = own_v[...]
    ring_gather(n, me, (own_k, own_v), (gk, gv), send, recv)

    def drain(s, carry):
        for c in range(seqs):
            for d in range(2):
                slot = inbox[d].at[s, c]
                remote(slot, slot, rs.at[d, c, s], rr.at[d, c, s], "ctx", targets[d]).wait_send()
        return carry

    lax.fori_loop(0, n - 1, drain, 0)


def reduce_gather(n, key_terms, value_terms, cosine, sine_back):
    _, seqs, rows, width = key_terms.shape
    kv = jax.ShapeDtypeStruct(key_terms.shape, BF16)
    sems = pltpu.SemaphoreType.DMA((2, seqs, n - 1))
    return pl.pallas_call(
        functools.partial(reduce_kernel, n),
        out_shape=(kv, kv),
        in_specs=[VMEM] * 4,
        out_specs=[VMEM] * 2,
        scratch_shapes=[
            pltpu.VMEM((n - 1, seqs, rows, width), BF16),
            pltpu.VMEM((n - 1, seqs, rows, width), BF16),
            pltpu.VMEM((seqs, rows, width), BF16),
            pltpu.VMEM((seqs, rows, width), BF16),
            sems,
            sems,
            sems,
            sems,
        ],
        compiler_params=pltpu.CompilerParams(
            collective_id=1, has_side_effects=True, vmem_limit_bytes=LIMIT
        ),
        name="reduce_kv",
    )(key_terms, value_terms, cosine, sine_back)


def scatter_kernel(m, part, out, near, held, far, send, recv):
    me = lax.axis_index("dp")
    greet("dp", m, me)
    half = m // 2
    pair = me + 1 - 2 * (me % 2)

    def first(j):
        to = (me // 2 + j) % half
        return remote(
            part.at[2 * to + pair % 2], near.at[j], send.at[j], recv.at[j], "dp", pair
        )

    def second(j):
        to = 2 * ((me // 2 + j) % half) + me % 2
        at = half + j - 1
        return remote(held.at[j - 1], far.at[j - 1], send.at[at], recv.at[at], "dp", to)

    order = list(range(1, half)) + [0]
    for j in order:
        first(j).start()
    for j in order:
        to = (me // 2 + j) % half
        first(j).wait_recv()
        both = part[2 * to + me % 2].astype(F32) + near[j].astype(F32)
        if j:
            held[j - 1] = both.astype(BF16)
            second(j).start()
        else:
            out[...] = both
    for j in range(1, half):
        second(j).wait_recv()
        out[...] += far[j - 1].astype(F32)
    for j in range(half):
        first(j).wait_send()
    for j in range(1, half):
        second(j).wait_send()


def scatter(m, part):
    _, rows, width = part.shape
    half = m // 2
    return pl.pallas_call(
        functools.partial(scatter_kernel, m),
        out_shape=jax.ShapeDtypeStruct((rows, width), F32),
        in_specs=[VMEM],
        out_specs=VMEM,
        scratch_shapes=[
            pltpu.VMEM((half, rows, width), BF16),
            pltpu.VMEM((max(half - 1, 1), rows, width), BF16),
            pltpu.VMEM((max(half - 1, 1), rows, width), BF16),
            pltpu.SemaphoreType.DMA((2 * half,)),
            pltpu.SemaphoreType.DMA((2 * half,)),
        ],
        compiler_params=pltpu.CompilerParams(
            collective_id=2, has_side_effects=True, vmem_limit_bytes=LIMIT
        ),
        name="scatter_weights",
    )(part)


def body(n, m, tokens, queries, d_attended, span_order, norm_gain, key_weight, value_weight):
    seqs, rows, model_width = tokens.shape
    kv_width = key_weight.shape[1]
    me = lax.axis_index("ctx")
    dp = lax.axis_index("dp")
    token_pos = positions(span_order, rows // 2)
    query_pos = lax.dynamic_slice_in_dim(token_pos, me * rows, rows, 0)
    cosine, sine = rotation(query_pos, HEAD_DIM)
    signs = jnp.where(jnp.arange(HEAD_DIM) < HEAD_DIM // 2, -1.0, 1.0).astype(F32)
    flat = tokens.reshape(seqs * rows, model_width)
    widened = flat.astype(F32)
    rms_scale = lax.rsqrt(jnp.mean(widened * widened, axis=-1, keepdims=True) + EPSILON)
    normed = (widened * rms_scale * norm_gain).astype(BF16)
    key_pre = jnp.dot(normed, key_weight, preferred_element_type=F32)
    key_pre = key_pre.reshape(seqs, rows, kv_width // HEAD_DIM, HEAD_DIM)
    turned = jnp.roll(key_pre, HEAD_DIM // 2, axis=-1)
    keys = key_pre * cosine[None, :, None, :] + turned * (sine * signs)[None, :, None, :]
    keys = keys.reshape(seqs, rows, kv_width).astype(BF16)
    values = jnp.dot(normed, value_weight, preferred_element_type=F32)
    values = values.reshape(seqs, rows, kv_width).astype(BF16)

    all_keys, all_values, slices = gather(n, keys, values, normed)
    attended, dquery, key_terms, value_terms = attention(
        queries, d_attended, all_keys, all_values, query_pos, token_pos
    )
    key_back, value_back = reduce_gather(n, key_terms, value_terms, cosine, -sine * signs)

    own_key = lax.dynamic_index_in_dim(key_back, me, 0, False).reshape(seqs * rows, kv_width)
    own_value = lax.dynamic_index_in_dim(value_back, me, 0, False).reshape(seqs * rows, kv_width)
    normed_grad = jnp.dot(own_key, key_weight.T, preferred_element_type=F32) + jnp.dot(
        own_value, value_weight.T, preferred_element_type=F32
    )
    inner_mean = jnp.mean(normed_grad * norm_gain * widened, axis=-1, keepdims=True)
    grad_rows = (
        rms_scale * norm_gain * normed_grad - widened * rms_scale**3 * inner_mean
    ).astype(BF16)

    stacked = slices.reshape(n * seqs * rows, model_width // n)
    weight_key = jnp.dot(
        stacked.T, key_back.reshape(n * seqs * rows, kv_width), preferred_element_type=F32
    )
    weight_value = jnp.dot(
        stacked.T, value_back.reshape(n * seqs * rows, kv_width), preferred_element_type=F32
    )
    own_rows = model_width // (n * m)
    part = jnp.concatenate([weight_key.astype(BF16), weight_value.astype(BF16)], axis=1)
    summed = scatter(m, part.reshape(m, own_rows, 2 * kv_width))
    grad_key_weight = summed[:, :kv_width]
    grad_value_weight = summed[:, kv_width:]
    start = (me * m + dp) * own_rows
    own_kw = lax.dynamic_slice_in_dim(key_weight, start, own_rows, 0).astype(F32)
    own_vw = lax.dynamic_slice_in_dim(value_weight, start, own_rows, 0).astype(F32)
    gain = lax.dynamic_slice_in_dim(norm_gain, start, own_rows, 0)
    grad_gain = jnp.sum(own_kw * grad_key_weight + own_vw * grad_value_weight, axis=1) / gain
    return (
        attended,
        dquery,
        grad_rows.reshape(seqs, rows, model_width),
        grad_key_weight,
        grad_value_weight,
        grad_gain,
    )


def solution(mesh):
    split = P("dp", "ctx", None)
    return jax.shard_map(
        functools.partial(body, mesh.shape["ctx"], mesh.shape["dp"]),
        mesh=mesh,
        in_specs=(split, split, split, P(), P(), P(), P()),
        out_specs=(
            split,
            split,
            split,
            P(("ctx", "dp"), None),
            P(("ctx", "dp"), None),
            P(("ctx", "dp")),
        ),
        check_vma=False,
    )
```

```python
import functools

import jax
import jax.numpy as jnp
from jax import lax
from jax.experimental import pallas as pl
from jax.experimental.pallas import tpu as pltpu
from jax.sharding import PartitionSpec as P

KV_HEADS = 4
HEAD_DIM = 128
ROPE_BASE = 500000.0
EPSILON = 1e-05
MESH = pl.DeviceIdType.MESH
VMEM = pl.BlockSpec(memory_space=pltpu.VMEM)
F32 = jnp.float32
BF16 = jnp.bfloat16
LIMIT = 60 * 1024 * 1024


def positions(span_order, span_len):
    offsets = jnp.arange(span_len, dtype=jnp.int32)
    return (span_order[:, None] * span_len + offsets[None, :]).reshape(-1)


def rotation(token_pos, head_size):
    half_dim = head_size // 2
    frequency = ROPE_BASE ** (-2.0 * jnp.arange(half_dim, dtype=F32) / head_size)
    angles = token_pos.astype(F32)[:, None] * frequency[None, :]
    angles = jnp.concatenate([angles, angles], axis=1)
    return (jnp.cos(angles), jnp.sin(angles))


def ring_place(index, n):
    return jnp.where(index % 2 == 0, index // 2, n - 1 - index // 2)


def ring_index(place, n):
    place = (place + 2 * n) % n
    return jnp.where(place < n // 2, 2 * place, 2 * (n - 1 - place) + 1)


def remote(src, dst, send, recv, axis, target):
    return pltpu.make_async_remote_copy(
        src_ref=src,
        dst_ref=dst,
        send_sem=send,
        recv_sem=recv,
        device_id={axis: target},
        device_id_type=MESH,
    )


def greet(axis, n, me):
    barrier = pltpu.get_barrier_semaphore()
    for j in range(1, n):
        pl.semaphore_signal(
            barrier, inc=1, device_id={axis: (me + j) % n}, device_id_type=MESH
        )
    pl.semaphore_wait(barrier, n - 1)


def ring_hops(n, d, t):
    return n // 2 if d == t else n // 2 - 1


def ring_gather(n, me, firsts, alls, send, recv, extra):
    place = ring_place(me, n)
    sign = (1, -1)
    targets = [ring_index(place + 1, n), ring_index(place - 1, n)]
    chunks = firsts[0].shape[0]
    lanes = [(c, t, d) for c in range(chunks) for t in range(2) for d in range(2)]

    def copy(d, t, c, s):
        owner = ring_index(place - sign[d] * s, n)
        src = firsts[t].at[c] if s == 0 else alls[t].at[owner, c]
        return remote(
            src,
            alls[t].at[owner, c],
            send.at[d, t, c, s],
            recv.at[d, t, c, s],
            "ctx",
            targets[d],
        )

    def arrive(d, t, c, s):
        owner = ring_index(place - sign[d] * (s + 1), n)
        slot = alls[t].at[owner, c]
        remote(
            slot, slot, send.at[d, t, c, s], recv.at[d, t, c, s], "ctx", targets[d]
        ).wait_recv()

    for s in range(n // 2):
        for c, t, d in lanes:
            if s < ring_hops(n, d, t):
                if s > 0:
                    arrive(d, t, c, s - 1)
                copy(d, t, c, s).start()
        extra(s)
    for c, t, d in lanes:
        hops = ring_hops(n, d, t)
        arrive(d, t, c, hops - 1)
    for s in range(n // 2):
        for c, t, d in lanes:
            if s < ring_hops(n, d, t):
                copy(d, t, c, s).wait_send()


def load_weights(sources, targets, sems):
    pieces = sems.shape[1]
    rows = sources[0].shape[0] // pieces
    return [
        [
            pltpu.make_async_copy(
                sources[t].at[pl.ds(q * rows, rows)],
                targets[t].at[pl.ds(q * rows, rows)],
                sems.at[t, q],
            )
            for t in range(2)
        ]
        for q in range(pieces)
    ]


PIECES = 4


def gather_kernel(
    n,
    early,
    x_ref,
    gain_ref,
    wk_hbm,
    wv_hbm,
    cos_ref,
    sin_ref,
    gk,
    gv,
    ga,
    wk,
    wv,
    normed,
    own_k,
    own_v,
    wsem,
    send,
    recv,
    asend,
    arecv,
):
    me = lax.axis_index("ctx")
    width = ga.shape[2]
    seqs, rows, kv_width = own_k.shape
    model_width = x_ref.shape[1]
    piece_width = model_width // PIECES
    loads = load_weights((wk_hbm, wv_hbm), (wk, wv), wsem)
    for pair in loads:
        for load in pair:
            load.start()
    total = jnp.zeros((x_ref.shape[0], 1), F32)
    for q in range(PIECES):
        wide = x_ref[:, q * piece_width : (q + 1) * piece_width].astype(F32)
        total = total + jnp.sum(wide * wide, axis=1, keepdims=True)
    rms = lax.rsqrt(total / model_width + EPSILON)
    for q in range(PIECES):
        at = slice(q * piece_width, (q + 1) * piece_width)
        normed[:, at] = (x_ref[:, at].astype(F32) * rms * gain_ref[:, at]).astype(BF16)
    greet("ctx", n, me)

    def piece(j):
        target = (me + j) % n
        return remote(
            normed.at[:, pl.ds(pl.multiple_of(target * width, 128), width)],
            ga.at[me],
            asend.at[j - 1],
            arecv.at[j - 1],
            "ctx",
            target,
        )

    for j in range(1, 1 + early):
        piece(j).start()
    key = jnp.zeros((seqs * rows, kv_width), F32)
    value = jnp.zeros((seqs * rows, kv_width), F32)
    for q in range(PIECES):
        at = slice(q * piece_width, (q + 1) * piece_width)
        for load in loads[q]:
            load.wait()
        part = normed[:, at]
        key = key + jnp.dot(part, wk[at], preferred_element_type=F32)
        value = value + jnp.dot(part, wv[at], preferred_element_type=F32)
    for c in range(seqs):
        for h in range(kv_width // HEAD_DIM):
            at = slice(h * HEAD_DIM, (h + 1) * HEAD_DIM)
            head = key[c * rows : (c + 1) * rows, at]
            turned = pltpu.roll(head, HEAD_DIM // 2, 1)
            own_k[c, :, at] = (head * cos_ref[...] + turned * sin_ref[...]).astype(BF16)
        own_v[c] = value[c * rows : (c + 1) * rows].astype(BF16)

    later = list(range(1 + early, n))
    half = n // 2

    def extra(s):
        if s == 0:
            gk[me] = own_k[...]
            gv[me] = own_v[...]
            ga[me] = normed[:, pl.ds(pl.multiple_of(me * width, 128), width)]
        for i, j in enumerate(later):
            if i * half // len(later) == s:
                piece(j).start()

    ring_gather(n, me, (own_k, own_v), (gk, gv), send, recv, extra)
    for j in range(1, n):
        piece(j).wait_send()
        slot = ga.at[(me + n - j) % n]
        remote(slot, slot, asend.at[j - 1], arecv.at[j - 1], "ctx", (me + j) % n).wait_recv()


ANY = pl.BlockSpec(memory_space=pl.ANY)


def gather(n, tokens, norm_gain, key_weight, value_weight, cosine, sine, seqs):
    count, model_width = tokens.shape
    rows = count // seqs
    kv_width = key_weight.shape[1]
    kv = jax.ShapeDtypeStruct((n, seqs, rows, kv_width), BF16)
    sems = pltpu.SemaphoreType.DMA((2, 2, seqs, n // 2))
    return pl.pallas_call(
        functools.partial(gather_kernel, n, n // 2 - 1),
        out_shape=(kv, kv, jax.ShapeDtypeStruct((n, count, model_width // n), BF16)),
        in_specs=[VMEM, VMEM, ANY, ANY, VMEM, VMEM],
        out_specs=[VMEM] * 3,
        scratch_shapes=[
            pltpu.VMEM(key_weight.shape, BF16),
            pltpu.VMEM(value_weight.shape, BF16),
            pltpu.VMEM(tokens.shape, BF16),
            pltpu.VMEM((seqs, rows, kv_width), BF16),
            pltpu.VMEM((seqs, rows, kv_width), BF16),
            pltpu.SemaphoreType.DMA((2, PIECES)),
            sems,
            sems,
            pltpu.SemaphoreType.DMA((n - 1,)),
            pltpu.SemaphoreType.DMA((n - 1,)),
        ],
        compiler_params=pltpu.CompilerParams(
            collective_id=0, has_side_effects=True, vmem_limit_bytes=LIMIT
        ),
        name="gather_kv",
    )(tokens, norm_gain, key_weight, value_weight, cosine, sine)


def attention_kernel(q_ref, g_ref, k_ref, v_ref, qpos_ref, kpos_ref, att, dq, dk, dv):
    n, _, rows, head = k_ref.shape
    group = q_ref.shape[2] // head
    scale = head ** (-0.5)
    query = jnp.concatenate([q_ref[0, :, i * head : (i + 1) * head] for i in range(group)], axis=0)
    grad = jnp.concatenate([g_ref[0, :, i * head : (i + 1) * head] for i in range(group)], axis=0)
    key = k_ref[...].reshape(n * rows, head)
    value = v_ref[...].reshape(n * rows, head)
    nt = (((1,), (1,)), ((), ()))
    nn = (((1,), (0,)), ((), ()))
    tn = (((0,), (0,)), ((), ()))
    dot = functools.partial(lax.dot_general, preferred_element_type=F32)
    keep = kpos_ref[...] <= jnp.concatenate([qpos_ref[...]] * group, axis=0)
    scores = jnp.where(keep, dot(query, key, nt) * scale, -1e30)
    exponent = jnp.exp(scores - jnp.max(scores, axis=1, keepdims=True))
    probability = exponent * (1.0 / jnp.sum(exponent, axis=1, keepdims=True))
    rounded = probability.astype(BF16)
    attended = dot(rounded, value, nn).astype(BF16)
    delta = jnp.sum(grad.astype(F32) * attended.astype(F32), axis=1, keepdims=True)
    dscores = (probability * (dot(grad, value, nt) - delta)).astype(BF16)
    dquery = (dot(dscores, key, nn) * scale).astype(BF16)
    for i in range(group):
        att[0, :, i * head : (i + 1) * head] = attended[i * rows : (i + 1) * rows]
        dq[0, :, i * head : (i + 1) * head] = dquery[i * rows : (i + 1) * rows]
    dk[...] = (dot(dscores, query, tn) * scale).astype(BF16).reshape(n, 1, rows, head)
    dv[...] = dot(rounded, grad, tn).astype(BF16).reshape(n, 1, rows, head)


def attention(queries, grads, all_keys, all_values, query_pos, key_pos):
    n, seqs, rows, width = all_keys.shape
    kv_heads = width // HEAD_DIM
    wide = pl.BlockSpec((1, rows, queries.shape[2] // kv_heads), lambda s, h: (s, 0, h))
    narrow = pl.BlockSpec((n, 1, rows, HEAD_DIM), lambda s, h: (0, s, 0, h))
    return pl.pallas_call(
        attention_kernel,
        grid=(seqs, kv_heads),
        out_shape=(
            jax.ShapeDtypeStruct(queries.shape, BF16),
            jax.ShapeDtypeStruct(queries.shape, BF16),
            jax.ShapeDtypeStruct(all_keys.shape, BF16),
            jax.ShapeDtypeStruct(all_keys.shape, BF16),
        ),
        in_specs=[
            wide,
            wide,
            narrow,
            narrow,
            pl.BlockSpec((rows, 1), lambda s, h: (0, 0)),
            pl.BlockSpec((1, n * rows), lambda s, h: (0, 0)),
        ],
        out_specs=[wide, wide, narrow, narrow],
        compiler_params=pltpu.CompilerParams(vmem_limit_bytes=LIMIT),
        name="attention",
    )(queries, grads, all_keys, all_values, query_pos[:, None], key_pos[None, :])


def reduce_kernel(
    n,
    dk,
    dv,
    cos_ref,
    sin_ref,
    x_ref,
    gain_ref,
    wk_hbm,
    wv_hbm,
    gk,
    gv,
    gx,
    wk,
    wv,
    normed_grad,
    inbox,
    own_k,
    own_v,
    wsem,
    rs,
    rr,
    send,
    recv,
):
    me = lax.axis_index("ctx")
    place = ring_place(me, n)
    _, seqs, rows, kv_width = dk.shape
    count, model_width = x_ref.shape
    piece_width = model_width // PIECES
    sign = (1, -1)
    targets = [ring_index(place + 1, n), ring_index(place - 1, n)]
    terms = (dk, dv)
    loads = load_weights((wk_hbm, wv_hbm), (wk, wv), wsem)
    for pair in loads:
        for load in pair:
            load.start()
    greet("ctx", n, me)
    lanes = [(c, t, d) for c in range(seqs) for t in range(2) for d in range(2)]

    def copy(d, t, c, s):
        owner = ring_index(place + sign[d] * ring_hops(n, d, t), n)
        src = terms[t].at[owner, c] if s == 0 else inbox.at[d, t, s - 1, c]
        return remote(
            src,
            inbox.at[d, t, s, c],
            rs.at[d, t, c, s],
            rr.at[d, t, c, s],
            "ctx",
            targets[d],
        )

    def arrive(d, t, c, s):
        slot = inbox.at[d, t, s, c]
        remote(slot, slot, rs.at[d, t, c, s], rr.at[d, t, c, s], "ctx", targets[d]).wait_recv()

    for s in range(n // 2):
        for c, t, d in lanes:
            hops = ring_hops(n, d, t)
            if s < hops:
                if s > 0:
                    arrive(d, t, c, s - 1)
                    owner = ring_index(place + sign[d] * (hops - s), n)
                    inbox[d, t, s - 1, c] = (
                        inbox[d, t, s - 1, c].astype(F32) + terms[t][owner, c].astype(F32)
                    ).astype(BF16)
                copy(d, t, c, s).start()

    def total(t, c):
        result = terms[t][me, c].astype(F32)
        for d in (1 - t, t):
            last = ring_hops(n, d, t) - 1
            arrive(d, t, c, last)
            result = result + inbox[d, t, last, c].astype(F32)
        return result

    for c in range(seqs):
        key_grad = total(0, c)
        for h in range(kv_width // HEAD_DIM):
            at = slice(h * HEAD_DIM, (h + 1) * HEAD_DIM)
            turned = pltpu.roll(key_grad[:, at], HEAD_DIM // 2, 1)
            back = key_grad[:, at] * cos_ref[...] + turned * sin_ref[...]
            own_k[c, :, at] = back.astype(BF16)
        own_v[c] = total(1, c).astype(BF16)

    state = {}

    def project(q):
        at = slice(q * piece_width, (q + 1) * piece_width)
        for load in loads[q]:
            load.wait()
        nt = (((1,), (1,)), ((), ()))
        part = lax.dot_general(
            own_k[...].reshape(count, kv_width), wk[at], nt, preferred_element_type=F32
        ) + lax.dot_general(
            own_v[...].reshape(count, kv_width), wv[at], nt, preferred_element_type=F32
        )
        normed_grad[:, at] = part
        wide = x_ref[:, at].astype(F32)
        square = jnp.sum(wide * wide, axis=1, keepdims=True)
        inner = jnp.sum(part * gain_ref[:, at] * wide, axis=1, keepdims=True)
        state["square"] = state["square"] + square if q else square
        state["inner"] = state["inner"] + inner if q else inner

    def finish():
        rms = lax.rsqrt(state["square"] / model_width + EPSILON)
        slope = rms * rms * rms * (state["inner"] / model_width)
        for q in range(PIECES):
            at = slice(q * piece_width, (q + 1) * piece_width)
            wide = x_ref[:, at].astype(F32)
            gx[:, at] = (rms * gain_ref[:, at] * normed_grad[:, at] - wide * slope).astype(BF16)

    def extra(s):
        if s == 0:
            gk[me] = own_k[...]
            gv[me] = own_v[...]
        for q in range(PIECES):
            if q * (n // 2) // PIECES == s:
                project(q)
                if q == PIECES - 1:
                    finish()

    ring_gather(n, me, (own_k, own_v), (gk, gv), send, recv, extra)
    for s in range(n // 2):
        for c, t, d in lanes:
            if s < ring_hops(n, d, t):
                copy(d, t, c, s).wait_send()


def reduce_gather(
    n, key_terms, value_terms, cosine, sine, tokens, norm_gain, key_weight, value_weight
):
    _, seqs, rows, width = key_terms.shape
    kv = jax.ShapeDtypeStruct(key_terms.shape, BF16)
    sems = pltpu.SemaphoreType.DMA((2, 2, seqs, n // 2))
    return pl.pallas_call(
        functools.partial(reduce_kernel, n),
        out_shape=(kv, kv, jax.ShapeDtypeStruct(tokens.shape, BF16)),
        in_specs=[VMEM] * 6 + [ANY] * 2,
        out_specs=[VMEM] * 3,
        scratch_shapes=[
            pltpu.VMEM(key_weight.shape, BF16),
            pltpu.VMEM(value_weight.shape, BF16),
            pltpu.VMEM(tokens.shape, F32),
            pltpu.VMEM((2, 2, n // 2, seqs, rows, width), BF16),
            pltpu.VMEM((seqs, rows, width), BF16),
            pltpu.VMEM((seqs, rows, width), BF16),
            pltpu.SemaphoreType.DMA((2, PIECES)),
            sems,
            sems,
            sems,
            sems,
        ],
        compiler_params=pltpu.CompilerParams(
            collective_id=1, has_side_effects=True, vmem_limit_bytes=LIMIT
        ),
        name="reduce_kv",
    )(key_terms, value_terms, cosine, sine, tokens, norm_gain, key_weight, value_weight)


def scatter_kernel(m, part, out, near, held, far, send, recv):
    me = lax.axis_index("dp")
    greet("dp", m, me)
    half = m // 2
    pair = me + 1 - 2 * (me % 2)

    def first(j):
        to = (me // 2 + j) % half
        return remote(
            part.at[2 * to + pair % 2], near.at[j], send.at[j], recv.at[j], "dp", pair
        )

    def second(j):
        to = 2 * ((me // 2 + j) % half) + me % 2
        at = half + j - 1
        return remote(held.at[j - 1], far.at[j - 1], send.at[at], recv.at[at], "dp", to)

    order = list(range(1, half)) + [0]
    for j in order:
        first(j).start()
    for j in order:
        to = (me // 2 + j) % half
        first(j).wait_recv()
        both = part[2 * to + me % 2].astype(F32) + near[j].astype(F32)
        if j:
            held[j - 1] = both.astype(BF16)
            second(j).start()
        else:
            out[...] = both
    for j in range(1, half):
        second(j).wait_recv()
        out[...] += far[j - 1].astype(F32)
    for j in range(half):
        first(j).wait_send()
    for j in range(1, half):
        second(j).wait_send()


def scatter(m, part):
    _, rows, width = part.shape
    half = m // 2
    return pl.pallas_call(
        functools.partial(scatter_kernel, m),
        out_shape=jax.ShapeDtypeStruct((rows, width), F32),
        in_specs=[VMEM],
        out_specs=VMEM,
        scratch_shapes=[
            pltpu.VMEM((half, rows, width), BF16),
            pltpu.VMEM((max(half - 1, 1), rows, width), BF16),
            pltpu.VMEM((max(half - 1, 1), rows, width), BF16),
            pltpu.SemaphoreType.DMA((2 * half,)),
            pltpu.SemaphoreType.DMA((2 * half,)),
        ],
        compiler_params=pltpu.CompilerParams(
            collective_id=2, has_side_effects=True, vmem_limit_bytes=LIMIT
        ),
        name="scatter_weights",
    )(part)


def body(n, m, tokens, queries, d_attended, span_order, norm_gain, key_weight, value_weight):
    seqs, rows, model_width = tokens.shape
    kv_width = key_weight.shape[1]
    me = lax.axis_index("ctx")
    dp = lax.axis_index("dp")
    token_pos = positions(span_order, rows // 2)
    query_pos = lax.dynamic_slice_in_dim(token_pos, me * rows, rows, 0)
    cosine, sine = rotation(query_pos, HEAD_DIM)
    signs = jnp.where(jnp.arange(HEAD_DIM) < HEAD_DIM // 2, -1.0, 1.0).astype(F32)
    flat = tokens.reshape(seqs * rows, model_width)
    row_gain = norm_gain[None, :]
    all_keys, all_values, slices = gather(
        n, flat, row_gain, key_weight, value_weight, cosine, sine * signs, seqs
    )
    attended, dquery, key_terms, value_terms = attention(
        queries, d_attended, all_keys, all_values, query_pos, token_pos
    )
    key_back, value_back, grad_rows = reduce_gather(
        n,
        key_terms,
        value_terms,
        cosine,
        -sine * signs,
        flat,
        row_gain,
        key_weight,
        value_weight,
    )

    stacked = slices.reshape(n * seqs * rows, model_width // n)
    weight_key = jnp.dot(
        stacked.T, key_back.reshape(n * seqs * rows, kv_width), preferred_element_type=F32
    )
    weight_value = jnp.dot(
        stacked.T, value_back.reshape(n * seqs * rows, kv_width), preferred_element_type=F32
    )
    own_rows = model_width // (n * m)
    part = jnp.concatenate([weight_key.astype(BF16), weight_value.astype(BF16)], axis=1)
    summed = scatter(m, part.reshape(m, own_rows, 2 * kv_width))
    grad_key_weight = summed[:, :kv_width]
    grad_value_weight = summed[:, kv_width:]
    start = (me * m + dp) * own_rows
    own_kw = lax.dynamic_slice_in_dim(key_weight, start, own_rows, 0).astype(F32)
    own_vw = lax.dynamic_slice_in_dim(value_weight, start, own_rows, 0).astype(F32)
    gain = lax.dynamic_slice_in_dim(norm_gain, start, own_rows, 0)
    grad_gain = jnp.sum(own_kw * grad_key_weight + own_vw * grad_value_weight, axis=1) / gain
    return (
        attended,
        dquery,
        grad_rows.reshape(seqs, rows, model_width),
        grad_key_weight,
        grad_value_weight,
        grad_gain,
    )


def solution(mesh):
    split = P("dp", "ctx", None)
    return jax.shard_map(
        functools.partial(body, mesh.shape["ctx"], mesh.shape["dp"]),
        mesh=mesh,
        in_specs=(split, split, split, P(), P(), P(), P()),
        out_specs=(
            split,
            split,
            split,
            P(("ctx", "dp"), None),
            P(("ctx", "dp"), None),
            P(("ctx", "dp")),
        ),
        check_vma=False,
    )
```

```python
import functools

import jax
import jax.numpy as jnp
from jax import lax
from jax.experimental import pallas as pl
from jax.experimental.pallas import tpu as pltpu
from jax.sharding import PartitionSpec as P

KV_HEADS = 4
HEAD_DIM = 128
ROPE_BASE = 500000.0
EPSILON = 1e-05
MESH = pl.DeviceIdType.MESH
VMEM = pl.BlockSpec(memory_space=pltpu.VMEM)
F32 = jnp.float32
BF16 = jnp.bfloat16
LIMIT = 60 * 1024 * 1024


def positions(span_order, span_len):
    offsets = jnp.arange(span_len, dtype=jnp.int32)
    return (span_order[:, None] * span_len + offsets[None, :]).reshape(-1)


def rotation(token_pos, head_size):
    half_dim = head_size // 2
    frequency = ROPE_BASE ** (-2.0 * jnp.arange(half_dim, dtype=F32) / head_size)
    angles = token_pos.astype(F32)[:, None] * frequency[None, :]
    angles = jnp.concatenate([angles, angles], axis=1)
    return (jnp.cos(angles), jnp.sin(angles))


def ring_place(index, n):
    return jnp.where(index % 2 == 0, index // 2, n - 1 - index // 2)


def ring_index(place, n):
    place = (place + 2 * n) % n
    return jnp.where(place < n // 2, 2 * place, 2 * (n - 1 - place) + 1)


def remote(src, dst, send, recv, axis, target):
    return pltpu.make_async_remote_copy(
        src_ref=src,
        dst_ref=dst,
        send_sem=send,
        recv_sem=recv,
        device_id={axis: target},
        device_id_type=MESH,
    )


def greet(axis, n, me):
    for j in range(1, n):
        pl.semaphore_signal(
            pltpu.get_barrier_semaphore(),
            inc=1,
            device_id={axis: (me + j) % n},
            device_id_type=MESH,
        )


def greeted(n):
    pl.semaphore_wait(pltpu.get_barrier_semaphore(), n - 1)


def ring_hops(n, d, t):
    return n // 2 if d == t else n // 2 - 1


def ring_gather(n, me, firsts, alls, send, recv, extra):
    place = ring_place(me, n)
    sign = (1, -1)
    targets = [ring_index(place + 1, n), ring_index(place - 1, n)]
    chunks = firsts[0].shape[0]
    lanes = [(c, t, d) for c in range(chunks) for t in range(2) for d in range(2)]

    def copy(d, t, c, s):
        owner = ring_index(place - sign[d] * s, n)
        src = firsts[t].at[c] if s == 0 else alls[t].at[owner, c]
        return remote(
            src,
            alls[t].at[owner, c],
            send.at[d, t, c, s],
            recv.at[d, t, c, s],
            "ctx",
            targets[d],
        )

    def arrive(d, t, c, s):
        owner = ring_index(place - sign[d] * (s + 1), n)
        slot = alls[t].at[owner, c]
        remote(
            slot, slot, send.at[d, t, c, s], recv.at[d, t, c, s], "ctx", targets[d]
        ).wait_recv()

    for s in range(n // 2):
        for c, t, d in lanes:
            if s < ring_hops(n, d, t):
                if s > 0:
                    arrive(d, t, c, s - 1)
                copy(d, t, c, s).start()
        extra(s)
    for c, t, d in lanes:
        hops = ring_hops(n, d, t)
        arrive(d, t, c, hops - 1)
    for s in range(n // 2):
        for c, t, d in lanes:
            if s < ring_hops(n, d, t):
                copy(d, t, c, s).wait_send()


def load_weights(sources, targets, sems):
    pieces = sems.shape[1]
    rows = sources[0].shape[0] // pieces
    return [
        [
            pltpu.make_async_copy(
                sources[t].at[pl.ds(q * rows, rows)],
                targets[t].at[pl.ds(q * rows, rows)],
                sems.at[t, q],
            )
            for t in range(2)
        ]
        for q in range(pieces)
    ]


PIECES = 4


def attend_group(c, h, q_ref, g_ref, k_ref, v_ref, qpos_ref, kpos_ref, att, dq, dk, dv):
    n, _, rows, kv_width = k_ref.shape
    head = HEAD_DIM
    group = q_ref.shape[2] // kv_width
    scale = head ** (-0.5)
    at = pl.ds(pl.multiple_of(h * head, head), head)
    columns = [pl.ds(pl.multiple_of((h * group + i) * head, head), head) for i in range(group)]
    query = jnp.concatenate([q_ref[c, :, column] for column in columns], axis=0)
    grad = jnp.concatenate([g_ref[c, :, column] for column in columns], axis=0)
    key = k_ref[:, c, :, at].reshape(n * rows, head)
    value = v_ref[:, c, :, at].reshape(n * rows, head)
    nt = (((1,), (1,)), ((), ()))
    nn = (((1,), (0,)), ((), ()))
    tn = (((0,), (0,)), ((), ()))
    dot = functools.partial(lax.dot_general, preferred_element_type=F32)
    keep = kpos_ref[...] <= jnp.concatenate([qpos_ref[...]] * group, axis=0)
    scores = jnp.where(keep, dot(query, key, nt) * scale, -1e30)
    exponent = jnp.exp(scores - jnp.max(scores, axis=1, keepdims=True))
    probability = exponent * (1.0 / jnp.sum(exponent, axis=1, keepdims=True))
    rounded = probability.astype(BF16)
    attended = dot(rounded, value, nn).astype(BF16)
    delta = jnp.sum(grad.astype(F32) * attended.astype(F32), axis=1, keepdims=True)
    dscores = (probability * (dot(grad, value, nt) - delta)).astype(BF16)
    dquery = (dot(dscores, key, nn) * scale).astype(BF16)
    for i in range(group):
        att[c, :, columns[i]] = attended[i * rows : (i + 1) * rows]
        dq[c, :, columns[i]] = dquery[i * rows : (i + 1) * rows]
    dk[:, c, :, at] = (dot(dscores, query, tn) * scale).astype(BF16).reshape(n, rows, head)
    dv[:, c, :, at] = dot(rounded, grad, tn).astype(BF16).reshape(n, rows, head)


def gather_kernel(
    n,
    early,
    x_ref,
    gain_ref,
    wk_hbm,
    wv_hbm,
    cos_ref,
    sin_ref,
    q_ref,
    g_ref,
    qpos_ref,
    kpos_ref,
    ga,
    att,
    dq,
    dk,
    dv,
    gk,
    gv,
    wk,
    wv,
    normed,
    own_k,
    own_v,
    wsem,
    send,
    recv,
    asend,
    arecv,
):
    me = lax.axis_index("ctx")
    width = ga.shape[2]
    seqs, rows, kv_width = own_k.shape
    model_width = x_ref.shape[1]
    piece_width = model_width // PIECES
    loads = load_weights((wk_hbm, wv_hbm), (wk, wv), wsem)
    for pair in loads:
        for load in pair:
            load.start()
    greet("ctx", n, me)
    total = jnp.zeros((x_ref.shape[0], 1), F32)
    for q in range(PIECES):
        wide = x_ref[:, q * piece_width : (q + 1) * piece_width].astype(F32)
        total = total + jnp.sum(wide * wide, axis=1, keepdims=True)
    rms = lax.rsqrt(total / model_width + EPSILON)
    for q in range(PIECES):
        at = slice(q * piece_width, (q + 1) * piece_width)
        normed[:, at] = (x_ref[:, at].astype(F32) * rms * gain_ref[:, at]).astype(BF16)
    greeted(n)

    def piece(j):
        target = (me + j) % n
        return remote(
            normed.at[:, pl.ds(pl.multiple_of(target * width, 128), width)],
            ga.at[me],
            asend.at[j - 1],
            arecv.at[j - 1],
            "ctx",
            target,
        )

    for j in range(1, 1 + early):
        piece(j).start()
    key = jnp.zeros((seqs * rows, kv_width), F32)
    value = jnp.zeros((seqs * rows, kv_width), F32)
    for q in range(PIECES):
        at = slice(q * piece_width, (q + 1) * piece_width)
        for load in loads[q]:
            load.wait()
        part = normed[:, at]
        key = key + jnp.dot(part, wk[at], preferred_element_type=F32)
        value = value + jnp.dot(part, wv[at], preferred_element_type=F32)
    for c in range(seqs):
        for h in range(kv_width // HEAD_DIM):
            at = slice(h * HEAD_DIM, (h + 1) * HEAD_DIM)
            head = key[c * rows : (c + 1) * rows, at]
            turned = pltpu.roll(head, HEAD_DIM // 2, 1)
            own_k[c, :, at] = (head * cos_ref[...] + turned * sin_ref[...]).astype(BF16)
        own_v[c] = value[c * rows : (c + 1) * rows].astype(BF16)

    later = list(range(1 + early, n))
    half = n // 2

    def extra(s):
        if s == 0:
            gk[me] = own_k[...]
            gv[me] = own_v[...]
            ga[me] = normed[:, pl.ds(pl.multiple_of(me * width, 128), width)]
        if s == half - 1:
            for j in later:
                piece(j).start()

    ring_gather(n, me, (own_k, own_v), (gk, gv), send, recv, extra)
    kv_heads = kv_width // HEAD_DIM

    def attend(i, carry):
        attend_group(i // kv_heads, i % kv_heads, q_ref, g_ref, gk, gv, qpos_ref, kpos_ref, att, dq, dk, dv)
        return carry

    lax.fori_loop(0, seqs * kv_heads, attend, 0)
    for j in range(1, n):
        piece(j).wait_send()
        slot = ga.at[(me + n - j) % n]
        remote(slot, slot, asend.at[j - 1], arecv.at[j - 1], "ctx", (me + j) % n).wait_recv()


ANY = pl.BlockSpec(memory_space=pl.ANY)


def gather_attend(n, tokens, norm_gain, key_weight, value_weight, cosine, sine, queries, grads, query_pos, key_pos):
    count, model_width = tokens.shape
    seqs, rows, _ = queries.shape
    kv_width = key_weight.shape[1]
    kv = (n, seqs, rows, kv_width)
    sems = pltpu.SemaphoreType.DMA((2, 2, seqs, n // 2))
    return pl.pallas_call(
        functools.partial(gather_kernel, n, n // 2 - 1),
        out_shape=(
            jax.ShapeDtypeStruct((n, count, model_width // n), BF16),
            jax.ShapeDtypeStruct(queries.shape, BF16),
            jax.ShapeDtypeStruct(queries.shape, BF16),
            jax.ShapeDtypeStruct(kv, BF16),
            jax.ShapeDtypeStruct(kv, BF16),
        ),
        in_specs=[VMEM, VMEM, ANY, ANY] + [VMEM] * 6,
        out_specs=[VMEM] * 5,
        scratch_shapes=[
            pltpu.VMEM(kv, BF16),
            pltpu.VMEM(kv, BF16),
            pltpu.VMEM(key_weight.shape, BF16),
            pltpu.VMEM(value_weight.shape, BF16),
            pltpu.VMEM(tokens.shape, BF16),
            pltpu.VMEM((seqs, rows, kv_width), BF16),
            pltpu.VMEM((seqs, rows, kv_width), BF16),
            pltpu.SemaphoreType.DMA((2, PIECES)),
            sems,
            sems,
            pltpu.SemaphoreType.DMA((n - 1,)),
            pltpu.SemaphoreType.DMA((n - 1,)),
        ],
        compiler_params=pltpu.CompilerParams(
            collective_id=0, has_side_effects=True, vmem_limit_bytes=LIMIT
        ),
        name="gather_attend",
    )(
        tokens,
        norm_gain,
        key_weight,
        value_weight,
        cosine,
        sine,
        queries,
        grads,
        query_pos[:, None],
        key_pos[None, :],
    )


def reduce_kernel(
    n,
    dk,
    dv,
    cos_ref,
    sin_ref,
    x_ref,
    gain_ref,
    wk_hbm,
    wv_hbm,
    gk,
    gv,
    gx,
    wk,
    wv,
    normed_grad,
    inbox,
    own_k,
    own_v,
    wsem,
    rs,
    rr,
    send,
    recv,
):
    me = lax.axis_index("ctx")
    place = ring_place(me, n)
    _, seqs, rows, kv_width = dk.shape
    count, model_width = x_ref.shape
    piece_width = model_width // PIECES
    sign = (1, -1)
    targets = [ring_index(place + 1, n), ring_index(place - 1, n)]
    terms = (dk, dv)
    loads = load_weights((wk_hbm, wv_hbm), (wk, wv), wsem)
    for pair in loads:
        for load in pair:
            load.start()
    greet("ctx", n, me)
    greeted(n)
    lanes = [(c, t, d) for c in range(seqs) for t in range(2) for d in range(2)]

    def copy(d, t, c, s):
        owner = ring_index(place + sign[d] * ring_hops(n, d, t), n)
        src = terms[t].at[owner, c] if s == 0 else inbox.at[d, t, s - 1, c]
        return remote(
            src,
            inbox.at[d, t, s, c],
            rs.at[d, t, c, s],
            rr.at[d, t, c, s],
            "ctx",
            targets[d],
        )

    def arrive(d, t, c, s):
        slot = inbox.at[d, t, s, c]
        remote(slot, slot, rs.at[d, t, c, s], rr.at[d, t, c, s], "ctx", targets[d]).wait_recv()

    for s in range(n // 2):
        for c, t, d in lanes:
            hops = ring_hops(n, d, t)
            if s < hops:
                if s > 0:
                    arrive(d, t, c, s - 1)
                    owner = ring_index(place + sign[d] * (hops - s), n)
                    inbox[d, t, s - 1, c] = (
                        inbox[d, t, s - 1, c].astype(F32) + terms[t][owner, c].astype(F32)
                    ).astype(BF16)
                copy(d, t, c, s).start()

    def total(t, c):
        result = terms[t][me, c].astype(F32)
        for d in (1 - t, t):
            last = ring_hops(n, d, t) - 1
            arrive(d, t, c, last)
            result = result + inbox[d, t, last, c].astype(F32)
        return result

    for c in range(seqs):
        key_grad = total(0, c)
        for h in range(kv_width // HEAD_DIM):
            at = slice(h * HEAD_DIM, (h + 1) * HEAD_DIM)
            turned = pltpu.roll(key_grad[:, at], HEAD_DIM // 2, 1)
            back = key_grad[:, at] * cos_ref[...] + turned * sin_ref[...]
            own_k[c, :, at] = back.astype(BF16)
        own_v[c] = total(1, c).astype(BF16)

    state = {}

    def project(q):
        at = slice(q * piece_width, (q + 1) * piece_width)
        for load in loads[q]:
            load.wait()
        nt = (((1,), (1,)), ((), ()))
        part = lax.dot_general(
            own_k[...].reshape(count, kv_width), wk[at], nt, preferred_element_type=F32
        ) + lax.dot_general(
            own_v[...].reshape(count, kv_width), wv[at], nt, preferred_element_type=F32
        )
        normed_grad[:, at] = part
        wide = x_ref[:, at].astype(F32)
        square = jnp.sum(wide * wide, axis=1, keepdims=True)
        inner = jnp.sum(part * gain_ref[:, at] * wide, axis=1, keepdims=True)
        state["square"] = state["square"] + square if q else square
        state["inner"] = state["inner"] + inner if q else inner

    def finish():
        rms = lax.rsqrt(state["square"] / model_width + EPSILON)
        slope = rms * rms * rms * (state["inner"] / model_width)
        for q in range(PIECES):
            at = slice(q * piece_width, (q + 1) * piece_width)
            wide = x_ref[:, at].astype(F32)
            gx[:, at] = (rms * gain_ref[:, at] * normed_grad[:, at] - wide * slope).astype(BF16)

    def extra(s):
        if s == 0:
            gk[me] = own_k[...]
            gv[me] = own_v[...]
        for q in range(PIECES):
            if q * (n // 2) // PIECES == s:
                project(q)
                if q == PIECES - 1:
                    finish()

    ring_gather(n, me, (own_k, own_v), (gk, gv), send, recv, extra)
    for s in range(n // 2):
        for c, t, d in lanes:
            if s < ring_hops(n, d, t):
                copy(d, t, c, s).wait_send()


def reduce_gather(
    n, key_terms, value_terms, cosine, sine, tokens, norm_gain, key_weight, value_weight
):
    _, seqs, rows, width = key_terms.shape
    kv = jax.ShapeDtypeStruct(key_terms.shape, BF16)
    sems = pltpu.SemaphoreType.DMA((2, 2, seqs, n // 2))
    return pl.pallas_call(
        functools.partial(reduce_kernel, n),
        out_shape=(kv, kv, jax.ShapeDtypeStruct(tokens.shape, BF16)),
        in_specs=[VMEM] * 6 + [ANY] * 2,
        out_specs=[VMEM] * 3,
        scratch_shapes=[
            pltpu.VMEM(key_weight.shape, BF16),
            pltpu.VMEM(value_weight.shape, BF16),
            pltpu.VMEM(tokens.shape, F32),
            pltpu.VMEM((2, 2, n // 2, seqs, rows, width), BF16),
            pltpu.VMEM((seqs, rows, width), BF16),
            pltpu.VMEM((seqs, rows, width), BF16),
            pltpu.SemaphoreType.DMA((2, PIECES)),
            sems,
            sems,
            sems,
            sems,
        ],
        compiler_params=pltpu.CompilerParams(
            collective_id=1, has_side_effects=True, vmem_limit_bytes=LIMIT
        ),
        name="reduce_kv",
    )(key_terms, value_terms, cosine, sine, tokens, norm_gain, key_weight, value_weight)


def scatter_kernel(m, x_ref, k_ref, v_ref, out, part, near, held, far, send, recv):
    me = lax.axis_index("dp")
    greet("dp", m, me)
    half = m // 2
    pair = me + 1 - 2 * (me % 2)

    def first(j):
        to = (me // 2 + j) % half
        return remote(
            part.at[2 * to + pair % 2], near.at[j], send.at[j], recv.at[j], "dp", pair
        )

    def second(j):
        to = 2 * ((me // 2 + j) % half) + me % 2
        at = half + j - 1
        return remote(held.at[j - 1], far.at[j - 1], send.at[at], recv.at[at], "dp", to)

    count, kv_width = k_ref.shape[0] * k_ref.shape[1], k_ref.shape[2]
    rows = out.shape[0]

    def multiply(t):
        at = pl.ds(pl.multiple_of(t * rows, 128), rows)
        lhs = x_ref[:, :, at].reshape(count, rows)
        for ref, start in ((k_ref, 0), (v_ref, kv_width)):
            rhs = ref[...].reshape(count, kv_width)
            term = lax.dot_general(
                lhs, rhs, (((0,), (0,)), ((), ())), preferred_element_type=F32
            )
            part[t, :, start : start + kv_width] = term.astype(BF16)

    order = list(range(1, half)) + [0]
    for i, j in enumerate(order):
        multiply(2 * ((me // 2 + j) % half) + pair % 2)
        if i == 0:
            greeted(m)
        first(j).start()
    for j in order:
        multiply(2 * ((me // 2 + j) % half) + me % 2)
    for j in order:
        to = (me // 2 + j) % half
        first(j).wait_recv()
        both = part[2 * to + me % 2].astype(F32) + near[j].astype(F32)
        if j:
            held[j - 1] = both.astype(BF16)
            second(j).start()
        else:
            out[...] = both
    for j in range(1, half):
        second(j).wait_recv()
        out[...] += far[j - 1].astype(F32)
    for j in range(half):
        first(j).wait_send()
    for j in range(1, half):
        second(j).wait_send()


def scatter(m, slices, key_back, value_back):
    rows, width = slices.shape[2] // m, 2 * key_back.shape[2]
    half = m // 2
    return pl.pallas_call(
        functools.partial(scatter_kernel, m),
        out_shape=jax.ShapeDtypeStruct((rows, width), F32),
        in_specs=[VMEM] * 3,
        out_specs=VMEM,
        scratch_shapes=[
            pltpu.VMEM((m, rows, width), BF16),
            pltpu.VMEM((half, rows, width), BF16),
            pltpu.VMEM((max(half - 1, 1), rows, width), BF16),
            pltpu.VMEM((max(half - 1, 1), rows, width), BF16),
            pltpu.SemaphoreType.DMA((2 * half,)),
            pltpu.SemaphoreType.DMA((2 * half,)),
        ],
        compiler_params=pltpu.CompilerParams(
            collective_id=2, has_side_effects=True, vmem_limit_bytes=LIMIT
        ),
        name="scatter_weights",
    )(slices, key_back, value_back)


def body(n, m, tokens, queries, d_attended, span_order, norm_gain, key_weight, value_weight):
    seqs, rows, model_width = tokens.shape
    kv_width = key_weight.shape[1]
    me = lax.axis_index("ctx")
    dp = lax.axis_index("dp")
    token_pos = positions(span_order, rows // 2)
    query_pos = lax.dynamic_slice_in_dim(token_pos, me * rows, rows, 0)
    cosine, sine = rotation(query_pos, HEAD_DIM)
    signs = jnp.where(jnp.arange(HEAD_DIM) < HEAD_DIM // 2, -1.0, 1.0).astype(F32)
    flat = tokens.reshape(seqs * rows, model_width)
    row_gain = norm_gain[None, :]
    slices, attended, dquery, key_terms, value_terms = gather_attend(
        n,
        flat,
        row_gain,
        key_weight,
        value_weight,
        cosine,
        sine * signs,
        queries,
        d_attended,
        query_pos,
        token_pos,
    )
    key_back, value_back, grad_rows = reduce_gather(
        n,
        key_terms,
        value_terms,
        cosine,
        -sine * signs,
        flat,
        row_gain,
        key_weight,
        value_weight,
    )

    count = seqs * rows
    summed = scatter(
        m,
        slices,
        key_back.reshape(n, count, kv_width),
        value_back.reshape(n, count, kv_width),
    )
    own_rows = model_width // (n * m)
    grad_key_weight = summed[:, :kv_width]
    grad_value_weight = summed[:, kv_width:]
    start = (me * m + dp) * own_rows
    own_kw = lax.dynamic_slice_in_dim(key_weight, start, own_rows, 0).astype(F32)
    own_vw = lax.dynamic_slice_in_dim(value_weight, start, own_rows, 0).astype(F32)
    gain = lax.dynamic_slice_in_dim(norm_gain, start, own_rows, 0)
    grad_gain = jnp.sum(own_kw * grad_key_weight + own_vw * grad_value_weight, axis=1) / gain
    return (
        attended,
        dquery,
        grad_rows.reshape(seqs, rows, model_width),
        grad_key_weight,
        grad_value_weight,
        grad_gain,
    )


def solution(mesh):
    split = P("dp", "ctx", None)
    return jax.shard_map(
        functools.partial(body, mesh.shape["ctx"], mesh.shape["dp"]),
        mesh=mesh,
        in_specs=(split, split, split, P(), P(), P(), P()),
        out_specs=(
            split,
            split,
            split,
            P(("ctx", "dp"), None),
            P(("ctx", "dp"), None),
            P(("ctx", "dp")),
        ),
        check_vma=False,
    )
```

```python
import functools

import jax
import jax.numpy as jnp
from jax import lax
from jax.experimental import pallas as pl
from jax.experimental.pallas import tpu as pltpu
from jax.sharding import PartitionSpec as P

KV_HEADS = 4
HEAD_DIM = 128
ROPE_BASE = 500000.0
EPSILON = 1e-05
MESH = pl.DeviceIdType.MESH
VMEM = pl.BlockSpec(memory_space=pltpu.VMEM)
F32 = jnp.float32
BF16 = jnp.bfloat16
LIMIT = 60 * 1024 * 1024


def positions(span_order, span_len):
    offsets = jnp.arange(span_len, dtype=jnp.int32)
    return (span_order[:, None] * span_len + offsets[None, :]).reshape(-1)


def rotation(token_pos, head_size):
    half_dim = head_size // 2
    frequency = ROPE_BASE ** (-2.0 * jnp.arange(half_dim, dtype=F32) / head_size)
    angles = token_pos.astype(F32)[:, None] * frequency[None, :]
    angles = jnp.concatenate([angles, angles], axis=1)
    return (jnp.cos(angles), jnp.sin(angles))


def ring_place(index, n):
    return jnp.where(index % 2 == 0, index // 2, n - 1 - index // 2)


def ring_index(place, n):
    place = (place + 2 * n) % n
    return jnp.where(place < n // 2, 2 * place, 2 * (n - 1 - place) + 1)


def remote(src, dst, send, recv, axis, target):
    return pltpu.make_async_remote_copy(
        src_ref=src,
        dst_ref=dst,
        send_sem=send,
        recv_sem=recv,
        device_id={axis: target},
        device_id_type=MESH,
    )


def greet(axis, n, me):
    for j in range(1, n):
        pl.semaphore_signal(
            pltpu.get_barrier_semaphore(),
            inc=1,
            device_id={axis: (me + j) % n},
            device_id_type=MESH,
        )


def greeted(n):
    pl.semaphore_wait(pltpu.get_barrier_semaphore(), n - 1)


def ring_hops(n, d, t):
    return n // 2 if d == t else n // 2 - 1


def ring_gather(n, me, firsts, alls, send, recv, extra):
    place = ring_place(me, n)
    sign = (1, -1)
    targets = [ring_index(place + 1, n), ring_index(place - 1, n)]
    chunks = firsts[0].shape[0]
    lanes = [(c, t, d) for c in range(chunks) for t in range(2) for d in range(2)]

    def copy(d, t, c, s):
        owner = ring_index(place - sign[d] * s, n)
        src = firsts[t].at[c] if s == 0 else alls[t].at[owner, c]
        return remote(
            src,
            alls[t].at[owner, c],
            send.at[d, t, c, s],
            recv.at[d, t, c, s],
            "ctx",
            targets[d],
        )

    def arrive(d, t, c, s):
        owner = ring_index(place - sign[d] * (s + 1), n)
        slot = alls[t].at[owner, c]
        remote(
            slot, slot, send.at[d, t, c, s], recv.at[d, t, c, s], "ctx", targets[d]
        ).wait_recv()

    for s in range(n // 2):
        for c, t, d in lanes:
            if s < ring_hops(n, d, t):
                if s > 0:
                    arrive(d, t, c, s - 1)
                copy(d, t, c, s).start()
        extra(s)
    for c, t, d in lanes:
        hops = ring_hops(n, d, t)
        arrive(d, t, c, hops - 1)
    for s in range(n // 2):
        for c, t, d in lanes:
            if s < ring_hops(n, d, t):
                copy(d, t, c, s).wait_send()


def load_weights(sources, targets, sems):
    pieces = sems.shape[1]
    rows = sources[0].shape[0] // pieces
    return [
        [
            pltpu.make_async_copy(
                sources[t].at[pl.ds(q * rows, rows)],
                targets[t].at[pl.ds(q * rows, rows)],
                sems.at[t, q],
            )
            for t in range(2)
        ]
        for q in range(pieces)
    ]


PIECES = 4


def attend_group(c, h, q_ref, g_ref, k_ref, v_ref, qpos_ref, kpos_ref, att, dq, dk, dv):
    n, _, rows, kv_width = k_ref.shape
    head = HEAD_DIM
    group = q_ref.shape[2] // kv_width
    scale = head ** (-0.5)
    at = pl.ds(pl.multiple_of(h * head, head), head)
    columns = [pl.ds(pl.multiple_of((h * group + i) * head, head), head) for i in range(group)]
    query = jnp.concatenate([q_ref[c, :, column] for column in columns], axis=0)
    grad = jnp.concatenate([g_ref[c, :, column] for column in columns], axis=0)
    key = k_ref[:, c, :, at].reshape(n * rows, head)
    value = v_ref[:, c, :, at].reshape(n * rows, head)
    nt = (((1,), (1,)), ((), ()))
    nn = (((1,), (0,)), ((), ()))
    tn = (((0,), (0,)), ((), ()))
    dot = functools.partial(lax.dot_general, preferred_element_type=F32)
    keep = kpos_ref[...] <= jnp.concatenate([qpos_ref[...]] * group, axis=0)
    scores = jnp.where(keep, dot(query, key, nt) * scale, -1e30)
    exponent = jnp.exp(scores - jnp.max(scores, axis=1, keepdims=True))
    probability = exponent * (1.0 / jnp.sum(exponent, axis=1, keepdims=True))
    rounded = probability.astype(BF16)
    attended = dot(rounded, value, nn).astype(BF16)
    delta = jnp.sum(grad.astype(F32) * attended.astype(F32), axis=1, keepdims=True)
    dscores = (probability * (dot(grad, value, nt) - delta)).astype(BF16)
    dquery = (dot(dscores, key, nn) * scale).astype(BF16)
    for i in range(group):
        att[c, :, columns[i]] = attended[i * rows : (i + 1) * rows]
        dq[c, :, columns[i]] = dquery[i * rows : (i + 1) * rows]
    dk[:, c, :, at] = (dot(dscores, query, tn) * scale).astype(BF16).reshape(n, rows, head)
    dv[:, c, :, at] = dot(rounded, grad, tn).astype(BF16).reshape(n, rows, head)


def gather_kernel(
    n,
    early,
    x_ref,
    gain_ref,
    wk_hbm,
    wv_hbm,
    cos_ref,
    sin_ref,
    q_ref,
    g_ref,
    qpos_ref,
    kpos_ref,
    ga,
    att,
    dq,
    dk,
    dv,
    gk,
    gv,
    wk,
    wv,
    normed,
    own_k,
    own_v,
    wsem,
    send,
    recv,
    asend,
    arecv,
):
    me = lax.axis_index("ctx")
    width = ga.shape[2]
    seqs, rows, kv_width = own_k.shape
    model_width = x_ref.shape[1]
    piece_width = model_width // PIECES
    loads = load_weights((wk_hbm, wv_hbm), (wk, wv), wsem)
    for pair in loads:
        for load in pair:
            load.start()
    greet("ctx", n, me)
    total = jnp.zeros((x_ref.shape[0], 1), F32)
    for q in range(PIECES):
        wide = x_ref[:, q * piece_width : (q + 1) * piece_width].astype(F32)
        total = total + jnp.sum(wide * wide, axis=1, keepdims=True)
    rms = lax.rsqrt(total / model_width + EPSILON)
    for q in range(PIECES):
        at = slice(q * piece_width, (q + 1) * piece_width)
        normed[:, at] = (x_ref[:, at].astype(F32) * rms * gain_ref[:, at]).astype(BF16)
    greeted(n)

    def piece(j):
        target = (me + j) % n
        return remote(
            normed.at[:, pl.ds(pl.multiple_of(target * width, 128), width)],
            ga.at[me],
            asend.at[j - 1],
            arecv.at[j - 1],
            "ctx",
            target,
        )

    for j in range(1, 1 + early):
        piece(j).start()
    key = jnp.zeros((seqs * rows, kv_width), F32)
    value = jnp.zeros((seqs * rows, kv_width), F32)
    for q in range(PIECES):
        at = slice(q * piece_width, (q + 1) * piece_width)
        for load in loads[q]:
            load.wait()
        part = normed[:, at]
        key = key + jnp.dot(part, wk[at], preferred_element_type=F32)
        value = value + jnp.dot(part, wv[at], preferred_element_type=F32)
    for c in range(seqs):
        for h in range(kv_width // HEAD_DIM):
            at = slice(h * HEAD_DIM, (h + 1) * HEAD_DIM)
            head = key[c * rows : (c + 1) * rows, at]
            turned = pltpu.roll(head, HEAD_DIM // 2, 1)
            own_k[c, :, at] = (head * cos_ref[...] + turned * sin_ref[...]).astype(BF16)
        own_v[c] = value[c * rows : (c + 1) * rows].astype(BF16)

    later = list(range(1 + early, n))
    half = n // 2

    def extra(s):
        if s == 0:
            gk[me] = own_k[...]
            gv[me] = own_v[...]
            ga[me] = normed[:, pl.ds(pl.multiple_of(me * width, 128), width)]
        if s == half - 1:
            for j in later:
                piece(j).start()

    ring_gather(n, me, (own_k, own_v), (gk, gv), send, recv, extra)
    kv_heads = kv_width // HEAD_DIM

    def attend(i, carry):
        attend_group(i // kv_heads, i % kv_heads, q_ref, g_ref, gk, gv, qpos_ref, kpos_ref, att, dq, dk, dv)
        return carry

    lax.fori_loop(0, seqs * kv_heads, attend, 0, unroll=2)
    for j in range(1, n):
        piece(j).wait_send()
        slot = ga.at[(me + n - j) % n]
        remote(slot, slot, asend.at[j - 1], arecv.at[j - 1], "ctx", (me + j) % n).wait_recv()


ANY = pl.BlockSpec(memory_space=pl.ANY)


def gather_attend(n, tokens, norm_gain, key_weight, value_weight, cosine, sine, queries, grads, query_pos, key_pos):
    count, model_width = tokens.shape
    seqs, rows, _ = queries.shape
    kv_width = key_weight.shape[1]
    kv = (n, seqs, rows, kv_width)
    sems = pltpu.SemaphoreType.DMA((2, 2, seqs, n // 2))
    return pl.pallas_call(
        functools.partial(gather_kernel, n, n // 2 - 1),
        out_shape=(
            jax.ShapeDtypeStruct((n, count, model_width // n), BF16),
            jax.ShapeDtypeStruct(queries.shape, BF16),
            jax.ShapeDtypeStruct(queries.shape, BF16),
            jax.ShapeDtypeStruct(kv, BF16),
            jax.ShapeDtypeStruct(kv, BF16),
        ),
        in_specs=[VMEM, VMEM, ANY, ANY] + [VMEM] * 6,
        out_specs=[VMEM] * 5,
        scratch_shapes=[
            pltpu.VMEM(kv, BF16),
            pltpu.VMEM(kv, BF16),
            pltpu.VMEM(key_weight.shape, BF16),
            pltpu.VMEM(value_weight.shape, BF16),
            pltpu.VMEM(tokens.shape, BF16),
            pltpu.VMEM((seqs, rows, kv_width), BF16),
            pltpu.VMEM((seqs, rows, kv_width), BF16),
            pltpu.SemaphoreType.DMA((2, PIECES)),
            sems,
            sems,
            pltpu.SemaphoreType.DMA((n - 1,)),
            pltpu.SemaphoreType.DMA((n - 1,)),
        ],
        compiler_params=pltpu.CompilerParams(
            collective_id=0, has_side_effects=True, vmem_limit_bytes=LIMIT
        ),
        name="gather_attend",
    )(
        tokens,
        norm_gain,
        key_weight,
        value_weight,
        cosine,
        sine,
        queries,
        grads,
        query_pos[:, None],
        key_pos[None, :],
    )


def reduce_kernel(
    n,
    dk,
    dv,
    cos_ref,
    sin_ref,
    x_ref,
    gain_ref,
    wk_hbm,
    wv_hbm,
    gk,
    gv,
    gx,
    wk,
    wv,
    normed_grad,
    inbox,
    own_k,
    own_v,
    wsem,
    rs,
    rr,
    send,
    recv,
):
    me = lax.axis_index("ctx")
    place = ring_place(me, n)
    _, seqs, rows, kv_width = dk.shape
    count, model_width = x_ref.shape
    piece_width = model_width // PIECES
    sign = (1, -1)
    targets = [ring_index(place + 1, n), ring_index(place - 1, n)]
    terms = (dk, dv)
    loads = load_weights((wk_hbm, wv_hbm), (wk, wv), wsem)
    for pair in loads:
        for load in pair:
            load.start()
    greet("ctx", n, me)
    greeted(n)
    lanes = [(c, t, d) for c in range(seqs) for t in range(2) for d in range(2)]

    def copy(d, t, c, s):
        owner = ring_index(place + sign[d] * ring_hops(n, d, t), n)
        src = terms[t].at[owner, c] if s == 0 else inbox.at[d, t, s - 1, c]
        return remote(
            src,
            inbox.at[d, t, s, c],
            rs.at[d, t, c, s],
            rr.at[d, t, c, s],
            "ctx",
            targets[d],
        )

    def arrive(d, t, c, s):
        slot = inbox.at[d, t, s, c]
        remote(slot, slot, rs.at[d, t, c, s], rr.at[d, t, c, s], "ctx", targets[d]).wait_recv()

    for s in range(n // 2):
        for c, t, d in lanes:
            hops = ring_hops(n, d, t)
            if s < hops:
                if s > 0:
                    arrive(d, t, c, s - 1)
                    owner = ring_index(place + sign[d] * (hops - s), n)
                    inbox[d, t, s - 1, c] = (
                        inbox[d, t, s - 1, c].astype(F32) + terms[t][owner, c].astype(F32)
                    ).astype(BF16)
                copy(d, t, c, s).start()

    def total(t, c):
        result = terms[t][me, c].astype(F32)
        for d in (1 - t, t):
            last = ring_hops(n, d, t) - 1
            arrive(d, t, c, last)
            result = result + inbox[d, t, last, c].astype(F32)
        return result

    for c in range(seqs):
        key_grad = total(0, c)
        for h in range(kv_width // HEAD_DIM):
            at = slice(h * HEAD_DIM, (h + 1) * HEAD_DIM)
            turned = pltpu.roll(key_grad[:, at], HEAD_DIM // 2, 1)
            back = key_grad[:, at] * cos_ref[...] + turned * sin_ref[...]
            own_k[c, :, at] = back.astype(BF16)
        own_v[c] = total(1, c).astype(BF16)

    state = {}

    def project(q):
        at = slice(q * piece_width, (q + 1) * piece_width)
        for load in loads[q]:
            load.wait()
        nt = (((1,), (1,)), ((), ()))
        part = lax.dot_general(
            own_k[...].reshape(count, kv_width), wk[at], nt, preferred_element_type=F32
        ) + lax.dot_general(
            own_v[...].reshape(count, kv_width), wv[at], nt, preferred_element_type=F32
        )
        normed_grad[:, at] = part
        wide = x_ref[:, at].astype(F32)
        square = jnp.sum(wide * wide, axis=1, keepdims=True)
        inner = jnp.sum(part * gain_ref[:, at] * wide, axis=1, keepdims=True)
        state["square"] = state["square"] + square if q else square
        state["inner"] = state["inner"] + inner if q else inner

    def finish():
        rms = lax.rsqrt(state["square"] / model_width + EPSILON)
        slope = rms * rms * rms * (state["inner"] / model_width)
        for q in range(PIECES):
            at = slice(q * piece_width, (q + 1) * piece_width)
            wide = x_ref[:, at].astype(F32)
            gx[:, at] = (rms * gain_ref[:, at] * normed_grad[:, at] - wide * slope).astype(BF16)

    def extra(s):
        if s == 0:
            gk[me] = own_k[...]
            gv[me] = own_v[...]
        for q in range(PIECES):
            if q * (n // 2) // PIECES == s:
                project(q)
                if q == PIECES - 1:
                    finish()

    ring_gather(n, me, (own_k, own_v), (gk, gv), send, recv, extra)
    for s in range(n // 2):
        for c, t, d in lanes:
            if s < ring_hops(n, d, t):
                copy(d, t, c, s).wait_send()


def reduce_gather(
    n, key_terms, value_terms, cosine, sine, tokens, norm_gain, key_weight, value_weight
):
    _, seqs, rows, width = key_terms.shape
    kv = jax.ShapeDtypeStruct(key_terms.shape, BF16)
    sems = pltpu.SemaphoreType.DMA((2, 2, seqs, n // 2))
    return pl.pallas_call(
        functools.partial(reduce_kernel, n),
        out_shape=(kv, kv, jax.ShapeDtypeStruct(tokens.shape, BF16)),
        in_specs=[VMEM] * 6 + [ANY] * 2,
        out_specs=[VMEM] * 3,
        scratch_shapes=[
            pltpu.VMEM(key_weight.shape, BF16),
            pltpu.VMEM(value_weight.shape, BF16),
            pltpu.VMEM(tokens.shape, F32),
            pltpu.VMEM((2, 2, n // 2, seqs, rows, width), BF16),
            pltpu.VMEM((seqs, rows, width), BF16),
            pltpu.VMEM((seqs, rows, width), BF16),
            pltpu.SemaphoreType.DMA((2, PIECES)),
            sems,
            sems,
            sems,
            sems,
        ],
        compiler_params=pltpu.CompilerParams(
            collective_id=1, has_side_effects=True, vmem_limit_bytes=LIMIT
        ),
        name="reduce_kv",
    )(key_terms, value_terms, cosine, sine, tokens, norm_gain, key_weight, value_weight)


def scatter_kernel(m, x_ref, k_ref, v_ref, out, part, near, held, far, send, recv):
    me = lax.axis_index("dp")
    greet("dp", m, me)
    half = m // 2
    pair = me + 1 - 2 * (me % 2)

    def first(j):
        to = (me // 2 + j) % half
        return remote(
            part.at[2 * to + pair % 2], near.at[j], send.at[j], recv.at[j], "dp", pair
        )

    def second(j):
        to = 2 * ((me // 2 + j) % half) + me % 2
        at = half + j - 1
        return remote(held.at[j - 1], far.at[j - 1], send.at[at], recv.at[at], "dp", to)

    count, kv_width = k_ref.shape[0] * k_ref.shape[1], k_ref.shape[2]
    rows = out.shape[0]

    def multiply(t):
        at = pl.ds(pl.multiple_of(t * rows, 128), rows)
        lhs = x_ref[:, :, at].reshape(count, rows)
        for ref, start in ((k_ref, 0), (v_ref, kv_width)):
            rhs = ref[...].reshape(count, kv_width)
            term = lax.dot_general(
                lhs, rhs, (((0,), (0,)), ((), ())), preferred_element_type=F32
            )
            part[t, :, start : start + kv_width] = term.astype(BF16)

    order = list(range(1, half)) + [0]
    for i, j in enumerate(order):
        multiply(2 * ((me // 2 + j) % half) + pair % 2)
        if i == 0:
            greeted(m)
        first(j).start()
    for j in order:
        multiply(2 * ((me // 2 + j) % half) + me % 2)
    for j in order:
        to = (me // 2 + j) % half
        first(j).wait_recv()
        both = part[2 * to + me % 2].astype(F32) + near[j].astype(F32)
        if j:
            held[j - 1] = both.astype(BF16)
            second(j).start()
        else:
            out[...] = both
    for j in range(1, half):
        second(j).wait_recv()
        out[...] += far[j - 1].astype(F32)
    for j in range(half):
        first(j).wait_send()
    for j in range(1, half):
        second(j).wait_send()


def scatter(m, slices, key_back, value_back):
    rows, width = slices.shape[2] // m, 2 * key_back.shape[2]
    half = m // 2
    return pl.pallas_call(
        functools.partial(scatter_kernel, m),
        out_shape=jax.ShapeDtypeStruct((rows, width), F32),
        in_specs=[VMEM] * 3,
        out_specs=VMEM,
        scratch_shapes=[
            pltpu.VMEM((m, rows, width), BF16),
            pltpu.VMEM((half, rows, width), BF16),
            pltpu.VMEM((max(half - 1, 1), rows, width), BF16),
            pltpu.VMEM((max(half - 1, 1), rows, width), BF16),
            pltpu.SemaphoreType.DMA((2 * half,)),
            pltpu.SemaphoreType.DMA((2 * half,)),
        ],
        compiler_params=pltpu.CompilerParams(
            collective_id=2, has_side_effects=True, vmem_limit_bytes=LIMIT
        ),
        name="scatter_weights",
    )(slices, key_back, value_back)


def body(n, m, tokens, queries, d_attended, span_order, norm_gain, key_weight, value_weight):
    seqs, rows, model_width = tokens.shape
    kv_width = key_weight.shape[1]
    me = lax.axis_index("ctx")
    dp = lax.axis_index("dp")
    token_pos = positions(span_order, rows // 2)
    query_pos = lax.dynamic_slice_in_dim(token_pos, me * rows, rows, 0)
    cosine, sine = rotation(query_pos, HEAD_DIM)
    signs = jnp.where(jnp.arange(HEAD_DIM) < HEAD_DIM // 2, -1.0, 1.0).astype(F32)
    flat = tokens.reshape(seqs * rows, model_width)
    row_gain = norm_gain[None, :]
    slices, attended, dquery, key_terms, value_terms = gather_attend(
        n,
        flat,
        row_gain,
        key_weight,
        value_weight,
        cosine,
        sine * signs,
        queries,
        d_attended,
        query_pos,
        token_pos,
    )
    key_back, value_back, grad_rows = reduce_gather(
        n,
        key_terms,
        value_terms,
        cosine,
        -sine * signs,
        flat,
        row_gain,
        key_weight,
        value_weight,
    )

    count = seqs * rows
    summed = scatter(
        m,
        slices,
        key_back.reshape(n, count, kv_width),
        value_back.reshape(n, count, kv_width),
    )
    own_rows = model_width // (n * m)
    grad_key_weight = summed[:, :kv_width]
    grad_value_weight = summed[:, kv_width:]
    start = (me * m + dp) * own_rows
    own_kw = lax.dynamic_slice_in_dim(key_weight, start, own_rows, 0).astype(F32)
    own_vw = lax.dynamic_slice_in_dim(value_weight, start, own_rows, 0).astype(F32)
    gain = lax.dynamic_slice_in_dim(norm_gain, start, own_rows, 0)
    grad_gain = jnp.sum(own_kw * grad_key_weight + own_vw * grad_value_weight, axis=1) / gain
    return (
        attended,
        dquery,
        grad_rows.reshape(seqs, rows, model_width),
        grad_key_weight,
        grad_value_weight,
        grad_gain,
    )


def solution(mesh):
    split = P("dp", "ctx", None)
    return jax.shard_map(
        functools.partial(body, mesh.shape["ctx"], mesh.shape["dp"]),
        mesh=mesh,
        in_specs=(split, split, split, P(), P(), P(), P()),
        out_specs=(
            split,
            split,
            split,
            P(("ctx", "dp"), None),
            P(("ctx", "dp"), None),
            P(("ctx", "dp")),
        ),
        check_vma=False,
    )
```
